128 devices in a mesh: member: 8 (over y, z_lo), tile: 16 (over z_hi, x, core).
Axes of the slice: x: 4, y: 4, z: 4 (z_hi: 2, z_lo: 2; z = z_hi * 2 + z_lo), core: 2. Of those that a mesh axis runs over, the one named last changes fastest.
Arguments:
- northward_speed_field: float32 [32, 16, 128, 1024], P('member', None, 'tile'), may hold values from -6 to 6
- level_depth_extent: float32 [32, 16, 128, 1024], P('member', None, 'tile'), may hold values from 0.2 to 5
- potential_warmth_anomaly: float32 [32, 16, 128, 1024], P('member', None, 'tile'), may hold values from -6 to 6
- ocean_region_label: int32 [128, 1024], P('tile'), may hold values from 0 to 9
- zone_for_parallel: int32 [1024], replicated, may hold values from 0 to 15, never falling along the last dimension, each value on 1 to 128 neighbouring positions
Outputs:
- mean_psi: float32 [10, 16, 1024], P(None, None, ('member', 'tile'))
- mean_heat: float32 [10, 1024], P(None, ('member', 'tile'))
- covariance: float32 [16, 32, 32], replicated
The draws below stay inside these ranges and needn't reach their ends.
Inputs may be any that keep to these rules, and one draw needn't show every extreme that they name: `zone_for_parallel`: never falls along latitude; every band holds 1 to 128 latitudes.
All inputs are finite; a program needn't handle non-finite values.
Results may differ from the reference program's by a relative error of at most 0.00011.
Values sent between devices are 32-bit elements; how exact they have to be, the bound alone decides.
A program may use at most 128 MiB of HBM per device.

```python
import math
import jax
import jax.numpy as jnp
import numpy as np
from jax import lax

BASINS = 10
VERTICAL_LEVELS = 16
NBANDS = 16
RUN_REPLICAS = 32
EASTWARD_POINTS = 128
NORTHWARD_LINES = 1024


def set_ends(array, stream_key, least, high):
    extent = array.shape
    spot = [jax.random.randint(jax.random.fold_in(stream_key, axis), (), 0, extent[axis]) for axis in range(len(extent))]
    array = array.at[tuple(spot)].set(least)
    longest = extent.index(max(extent))
    spot[longest] = (spot[longest] + 1) % extent[longest]
    return array.at[tuple(spot)].set(high)


def block_levels(rng, shape, pieces, least, high):
    gain = 1.0
    for dim, shards_of in pieces:
        draws = jax.random.uniform(jax.random.fold_in(jax.random.fold_in(rng, 6), dim), (shards_of,), jnp.float32, least / len(pieces), high / len(pieces))
        gain = gain * jnp.repeat(jnp.exp(draws), shape[dim] // shards_of).reshape((-1,) + (1,) * (len(shape) - 1 - dim))
    return gain


def profile(amount, total, most, slope):
    loads = [(1 << 20) // math.isqrt(grade ** slope) + 1 for grade in range(2, amount + 1)]
    spare, holding = total - most - (amount - 1), [1] * (amount - 1)
    while spare > 0:
        movable = [i for i in range(amount - 1) if holding[i] < most]
        mass, budget = sum([loads[i] for i in movable]), spare
        for i in movable:
            extra = min(most - holding[i], max(1, budget * loads[i] // mass), spare)
            holding[i] = holding[i] + extra
            spare = spare - extra
    return np.array([most] + holding)


def ragged_sizes(stream_key, count, total, bound, lean):
    if count == 2:
        one = jax.random.randint(stream_key, (), max(1, total - bound), min(bound, total - 1) + 1)
        return jnp.stack([one, total - one])
    sizes = jnp.asarray(profile(count, total, bound, lean), jnp.int32)
    couples = (count - 1) // 2
    giver, sink = sizes[1:1 + 2 * couples:2], sizes[2:2 + 2 * couples:2]
    margin = jnp.minimum(giver - 1, bound - sink)
    moved = jax.random.randint(jax.random.fold_in(stream_key, 1), (couples,), 0, 1 << 20) % (margin + 1)
    sizes = sizes.at[1:1 + 2 * couples:2].set(giver - moved).at[2:2 + 2 * couples:2].set(sink + moved)
    return sizes[jax.random.permutation(jax.random.fold_in(stream_key, 2), count)]


def centred(stream_key, extent, deviation, bound, cuts=(), kind=jnp.bfloat16):
    loudness = block_levels(stream_key, extent, cuts, -0.22, 0.18) if cuts else 1.0
    values = jax.random.normal(stream_key, extent, jnp.float32) * deviation * loudness
    return jnp.minimum(jnp.maximum(values, -bound), bound).astype(kind)


def setup_inputs(seed: int = 0) -> dict:
    arg_keys = jax.random.split(jax.random.key(seed), 6)
    northward_speed_field = centred(arg_keys[0], (RUN_REPLICAS, VERTICAL_LEVELS, EASTWARD_POINTS, NORTHWARD_LINES), 1.0, 6.0, ((0, 8), (2, 16)), jnp.float32)
    level_depth_extent = jnp.clip(jnp.exp(math.log(5.0) - 3.218876 * jax.random.uniform(arg_keys[1], (RUN_REPLICAS, VERTICAL_LEVELS, EASTWARD_POINTS, NORTHWARD_LINES), jnp.float32) ** block_levels(arg_keys[1], (RUN_REPLICAS, VERTICAL_LEVELS, EASTWARD_POINTS, NORTHWARD_LINES), ((0, 8), (2, 16)), -0.2, 0.2)), 0.2, 5.0)
    potential_warmth_anomaly = centred(arg_keys[2], (RUN_REPLICAS, VERTICAL_LEVELS, EASTWARD_POINTS, NORTHWARD_LINES), 1.0, 6.0, ((0, 8), (2, 16)), jnp.float32)
    ocean_region_label = set_ends(jax.random.randint(arg_keys[3], (EASTWARD_POINTS, NORTHWARD_LINES), 0, BASINS), jax.random.fold_in(arg_keys[3], 1), 0, BASINS - 1).astype(jnp.int32)
    zone_for_parallel = jnp.searchsorted(jnp.cumsum(ragged_sizes(arg_keys[4], NBANDS, NORTHWARD_LINES, NORTHWARD_LINES // 8, 1)), jnp.arange(NORTHWARD_LINES), side="right").astype(jnp.int32)
    return {"northward_speed_field": northward_speed_field, "level_depth_extent": level_depth_extent, "potential_warmth_anomaly": potential_warmth_anomaly, "ocean_region_label": ocean_region_label, "zone_for_parallel": zone_for_parallel}


def metric_factor(lats):
    index = jnp.arange(lats, dtype=jnp.float32)
    return jnp.cos((-80.0 + 160.0 * (index + 0.5) / lats) * (math.pi / 180.0))

def reference(northward_speed_field, level_depth_extent, potential_warmth_anomaly, ocean_region_label, zone_for_parallel):
    greatest_bound_value = lax.Precision.HIGHEST
    northward_volume_carriage = northward_speed_field * level_depth_extent * metric_factor(NORTHWARD_LINES)
    region_indicator_matrix = (ocean_region_label[None, :, :] == jnp.arange(BASINS, dtype=jnp.int32)[:, None, None]).astype(jnp.float32)
    transport = jnp.einsum('mkxl,bxl->mbkl', northward_volume_carriage, region_indicator_matrix, precision=greatest_bound_value) / math.sqrt(EASTWARD_POINTS)
    thermal_energy_integral = jnp.einsum('tzux,pux->tpx', northward_volume_carriage * potential_warmth_anomaly, region_indicator_matrix, precision=greatest_bound_value) / math.sqrt(EASTWARD_POINTS * VERTICAL_LEVELS)
    stream = jnp.cumsum(transport, axis=2)
    mean_psi = lax.optimization_barrier(jnp.mean(stream, axis=0))
    mean_heat = lax.optimization_barrier(jnp.mean(thermal_energy_integral, axis=0))
    anomaly = (stream - mean_psi).reshape(RUN_REPLICAS, BASINS * VERTICAL_LEVELS, NORTHWARD_LINES)
    products = jnp.einsum('mfl,nfl->lmn', anomaly, anomaly, precision=greatest_bound_value)
    band_hot = (zone_for_parallel[:, None] == jnp.arange(NBANDS, dtype=jnp.int32)[None, :]).astype(jnp.float32)
    norm = float((RUN_REPLICAS - 1) * BASINS * VERTICAL_LEVELS * (NORTHWARD_LINES // NBANDS))
    covariance = jnp.einsum('lmn,lc->cmn', products, band_hot, precision=greatest_bound_value) / norm
    return (mean_psi, mean_heat, covariance)
```

```python
import math

import jax
import jax.numpy as jnp
from jax import lax
from jax.experimental import pallas as pl
from jax.experimental.pallas import tpu as pltpu
from jax.sharding import PartitionSpec as P

MESH = pl.DeviceIdType.MESH
F32 = jnp.float32
BF16 = jnp.bfloat16

LANES = 128
BASINS = 10
LAYERS = 16
NBANDS = 16
MEMBERS = 32
GROUPS = 8
MINE = MEMBERS // GROUPS
COLS = 8
ROWS = BASINS + 1
PAD = 16
RING = 4
PEERS = 8
SPREAD = 16


def metric_factor(lats):
    index = jnp.arange(lats, dtype=F32)
    return jnp.cos((-80.0 + 160.0 * (index + 0.5) / lats) * (math.pi / 180.0))


def kernel(
    v_hbm, h_hbm, t_hbm, lab_ref, zone_ref, sp_ref,
    psi_out, heat_out, cov_out,
    vb, hb, tb, onehot, heat_cols, ps, cr, xs, fa, fb, na, nb, rl, ys, rb,
    an, pp, dd, c1, s1, c2, s2, df, mb, mm,
    hbm_sem, core_s, core_r, x_s, x_r, yz_s, yz_r,
    c1_s, c1_r, c2_s, c2_r, c3_s, c3_r, m1_s, m1_r, m2_s, m2_r,
):
    member = lax.axis_index("member")
    tile = lax.axis_index("tile")
    z_hi = tile // PEERS
    e = tile % PEERS
    x = e // 2
    core = e % 2
    me = z_hi * GROUPS + member

    def peer(i):
        other = lax.rem(e + i, PEERS)
        return other, {"member": member, "tile": z_hi * PEERS + other}

    def spread(i):
        other = lax.rem(me + i, SPREAD)
        return other, {"member": other % GROUPS, "tile": (other // GROUPS) * PEERS + e}

    def along_x(step):
        other = lax.rem(x + RING + step, RING)
        return {"member": member, "tile": z_hi * PEERS + other * 2 + core}

    sibling = {"member": member, "tile": z_hi * PEERS + x * 2 + (1 - core)}

    def remote(src, dst, send, recv, device):
        return pltpu.make_async_remote_copy(
            src_ref=src, dst_ref=dst, send_sem=send, recv_sem=recv,
            device_id=device, device_id_type=MESH,
        )

    chunk = LAYERS * COLS * 8

    def load(m):
        rows = pl.ds(m * chunk, chunk)
        return [
            pltpu.make_async_copy(a.at[rows], b.at[rows], hbm_sem.at[m, i])
            for i, (a, b) in enumerate(((v_hbm, vb), (h_hbm, hb), (t_hbm, tb)))
        ]

    for m in range(2):
        for c in load(m):
            c.start()

    barrier = pltpu.get_barrier_semaphore()

    @pl.loop(1, PEERS)
    def _(i):
        pl.semaphore_signal(barrier, inc=1, device_id=peer(i)[1], device_id_type=MESH)

    @pl.loop(1, SPREAD)
    def _(i):
        pl.semaphore_signal(barrier, inc=1, device_id=spread(i)[1], device_id_type=MESH)

    for col in range(COLS):
        lab = lab_ref[pl.ds(col, 8, stride=8), :]
        for b in range(BASINS):
            onehot[col * BASINS + b] = jnp.where(lab == b, 1.0, 0.0).astype(F32)
    zero = jnp.zeros((8, LANES), F32)
    for col in range(COLS):
        heat_cols[col] = zero

    def rows_of(m):
        return ROWS if m == MINE - 1 else BASINS

    def compute(m):
        for c in load(m):
            c.wait()
        if m + 2 < MINE:
            for c in load(m + 2):
                c.start()

        def body(kk, carry):
            acc, hs = list(carry[0]), list(carry[1])
            nxt = [None] * BASINS
            for col in range(COLS):
                base = m * chunk + kk * (2 * COLS * 8) + col
                first = pl.ds(base, 8, stride=8)
                second = pl.ds(base + COLS * 8, 8, stride=8)
                u0 = vb[first, :] * hb[first, :]
                u1 = vb[second, :] * hb[second, :]
                hs[col] = hs[col] + (u0 * tb[first, :] + u1 * tb[second, :])
                for b in range(BASINS):
                    o = onehot[col * BASINS + b]
                    acc[b] = acc[b] + o * u0
                    nxt[b] = o * u1 if nxt[b] is None else nxt[b] + o * u1
            for b in range(BASINS):
                ps[m, 0, kk, b] = acc[b]
                acc[b] = acc[b] + nxt[b]
                ps[m, 1, kk, b] = acc[b]
            return tuple(acc), tuple(hs)

        start = (tuple(zero for _ in range(BASINS)), tuple(heat_cols[c] for c in range(COLS)))
        _, hs = lax.fori_loop(0, LAYERS // 2, body, start)
        if m < MINE - 1:
            for col in range(COLS):
                heat_cols[col] = hs[col]
        else:
            for k in range(LAYERS):
                row = zero
                if k < BASINS:
                    for col in range(COLS):
                        row = row + onehot[col * BASINS + k] * hs[col]
                ps[m, k % 2, k // 2, BASINS] = row

    def core_copy(m):
        n = rows_of(m)
        return remote(
            ps.at[m, 1 - core, :, pl.ds(0, n)], cr.at[m, :, pl.ds(0, n)],
            core_s.at[m], core_r.at[m], sibling,
        )

    right, left = along_x(1), along_x(-1)
    at_right = lax.rem(x + 1, RING)
    at_left = lax.rem(x + 3, RING)
    at_far = lax.rem(x + 2, RING)

    def x_copies(m):
        n = pl.ds(0, rows_of(m))
        hi = RING

        def c(i, src, dst, device):
            return lambda: remote(src, dst, x_s.at[m, i], x_r.at[m, i], device)

        return dict(
            far_right=c(0, xs.at[m, at_far, n], fa.at[m, n], right),
            far_left=c(1, xs.at[m, hi + at_far, n], fb.at[m, n], left),
            near_right=c(2, xs.at[m, hi + at_right, n], na.at[m, 1, n], right),
            near_left=c(3, xs.at[m, at_left, n], nb.at[m, 0, n], left),
            sum_right=c(4, rl.at[m, 0, n], na.at[m, 0, n], right),
            sum_left=c(5, rl.at[m, 1, n], nb.at[m, 1, n], left),
        )

    def pair_sum(m):
        core_copy(m).wait_recv()
        n = rows_of(m)

        def one(kk, _):
            for r in range(n):
                xs[m, kk, r] = ps[m, core, kk, r] + cr[m, kk, r]
            return 0

        copies = x_copies(m)
        lax.fori_loop(0, LAYERS // 2, one, 0)
        for name in ("far_right", "far_left", "near_right", "near_left"):
            copies[name]().start()

    def relay(m):
        copies = x_copies(m)
        n = rows_of(m)
        copies["far_right"]().wait_recv()
        for r in range(n):
            rl[m, 0, r] = xs[m, at_right, r] + fa[m, r]
        copies["sum_right"]().start()
        copies["far_left"]().wait_recv()
        for r in range(n):
            rl[m, 1, r] = xs[m, RING + at_left, r] + fb[m, r]
        copies["sum_left"]().start()

    def piece(ref, i):
        return ref.at[pl.ds(pl.multiple_of(i * PAD, PAD), PAD)]

    def spread_out(m):
        copies = x_copies(m)
        n = rows_of(m)
        for name in ("near_right", "near_left", "sum_right", "sum_left"):
            copies[name]().wait_recv()
        for z in range(2):
            for r in range(n):
                total = xs[m, z * RING + x, r] + (na[m, z, r] + nb[m, z, r])
                ys[pl.ds((m * SPREAD + z * GROUPS) * PAD + r, 8, stride=PAD), :] = total
        for r in range(n, PAD):
            for z in range(2):
                ys[pl.ds((m * SPREAD + z * GROUPS) * PAD + r, 8, stride=PAD), :] = zero

        @pl.loop(1, SPREAD)
        def _(i):
            other, device = spread(i)
            remote(
                piece(ys, m * SPREAD + other), piece(rb, me * MINE + m),
                yz_s.at[m], yz_r.at[m], device,
            ).start()

        piece(rb, me * MINE + m)[...] = piece(ys, m * SPREAD + me)[...]

    def wait_bytes(ref, rows, sem):
        view = ref.at[pl.ds(0, rows)]
        pltpu.make_async_copy(view, view, sem).wait()

    compute(0)
    pl.semaphore_wait(barrier, PEERS - 1 + SPREAD - 1)
    core_copy(0).start()
    compute(1)
    core_copy(1).start()
    pair_sum(0)
    compute(2)
    core_copy(2).start()
    pair_sum(1)
    relay(0)
    compute(3)
    core_copy(3).start()
    pair_sum(2)
    relay(1)
    pair_sum(3)
    spread_out(0)
    relay(2)
    spread_out(1)
    relay(3)
    spread_out(2)
    spread_out(3)
    for m in range(MINE):
        wait_bytes(ys, (SPREAD - 1) * PAD, yz_r.at[m])

    spacing = jnp.broadcast_to(sp_ref[pl.ds(member, 1), :], (8, LANES))
    for b in range(BASINS):
        a = []
        for q in range(4):
            lo = rb[pl.ds(q * 8 * PAD + b, 8, stride=PAD), :]
            hi = rb[pl.ds((MEMBERS + q * 8) * PAD + b, 8, stride=PAD), :]
            a.append((lo + hi) * spacing)
        mean = jnp.sum((a[0] + a[1]) + (a[2] + a[3]), axis=0, keepdims=True) * (1.0 / MEMBERS)
        mb[pl.ds(b, 1), :] = mean
        for q in range(4):
            an[pl.ds(b * MEMBERS + q * 8, 8), :] = a[q] - mean
    last = (MINE - 1) * PAD + BASINS
    warm = rb[pl.ds(last, 8, stride=MINE * PAD), :] + rb[
        pl.ds(last + GROUPS * MINE * PAD, 8, stride=MINE * PAD), :
    ]
    warm = jnp.sum(warm * spacing, axis=0, keepdims=True)
    mb[pl.ds(BASINS, 1), :] = warm * (1.0 / (MEMBERS * math.sqrt(LAYERS)))
    for r in range(ROWS, PAD):
        mb[pl.ds(r, 1), :] = jnp.zeros((1, LANES), F32)

    mm[pl.ds(pl.multiple_of((e * 2 + z_hi) * PAD, PAD), PAD), :] = mb[...]
    means_over = remote(
        mb, piece(mm, e * 2 + z_hi), m1_s, m1_r,
        {"member": member, "tile": (1 - z_hi) * PEERS + e},
    )
    means_over.start()

    def gram(n, _):
        acc = [None] * 4
        for b in range(BASINS):
            row = jnp.broadcast_to(an[pl.ds(b * MEMBERS + n, 1), :], (8, LANES))
            for q in range(4):
                t = row * an[pl.ds(b * MEMBERS + q * 8, 8), :]
                acc[q] = t if acc[q] is None else acc[q] + t
        at = pl.multiple_of((n % 8) * LANES + (n // 8) * MEMBERS, MEMBERS)
        for q in range(4):
            pp[pl.ds(at + q * 8, 8), :] = acc[q]
        return 0

    lax.fori_loop(0, MEMBERS, gram, 0)

    zone = jnp.broadcast_to(zone_ref[pl.ds(member, 1), :], (NBANDS, LANES))
    band = jnp.where(
        zone == lax.broadcasted_iota(jnp.int32, (NBANDS, LANES), 0), 1.0, 0.0
    ).astype(BF16)
    for r in range(8):
        p = pp[pl.ds(r * LANES, LANES), :]
        total = None
        for _ in range(3):
            part = p.astype(BF16)
            p = p - part.astype(F32)
            d = lax.dot_general(
                band, part, (((1,), (1,)), ((), ())), preferred_element_type=F32
            )
            total = d if total is None else total + d
        dd[pl.ds(r * PAD, PAD), :] = total

    @pl.loop(1, PEERS)
    def _(i):
        other, device = peer(i)
        remote(piece(dd, other), piece(c1, e), c1_s, c1_r, device).start()

    means_over.wait_recv()
    both = pl.ds(pl.multiple_of(e * 2 * PAD, PAD), 2 * PAD)

    @pl.loop(1, PEERS)
    def _(i):
        remote(mm.at[both], mm.at[both], m2_s, m2_r, peer(i)[1]).start()

    piece(c1, e)[...] = piece(dd, e)[...]
    wait_bytes(c1, (PEERS - 1) * PAD, c1_r)
    total = c1[pl.ds(0, PAD), :]
    for i in range(1, PEERS):
        total = total + c1[pl.ds(i * PAD, PAD), :]
    s1[...] = total

    @pl.loop(1, SPREAD)
    def _(i):
        remote(s1, piece(c2, me), c2_s, c2_r, spread(i)[1]).start()

    piece(c2, me)[...] = total

    wait_bytes(mm, (PEERS - 1) * 2 * PAD, m2_r)
    turn = lax.rem(LANES - tile * 8, LANES)

    def mine(rows):
        return pltpu.roll(rows, turn, 1)[:, :8]

    for b in range(BASINS):
        for z in range(2):
            rows = mm[pl.ds(z * PAD + b, 8, stride=2 * PAD), :]
            psi_out[b, pl.ds(z * 8, 8), :] = mine(rows)
    heat_out[pl.ds(0, 8), :] = mine(mm[pl.ds(BASINS, 8, stride=2 * PAD), :])
    heat_out[pl.ds(8, 2), :] = mine(mm[pl.ds(PAD + BASINS, 8, stride=2 * PAD), :])[:2]

    wait_bytes(c2, (SPREAD - 1) * PAD, c2_r)
    total = c2[pl.ds(0, PAD), :]
    for i in range(1, SPREAD):
        total = total + c2[pl.ds(i * PAD, PAD), :]
    norm = float((MEMBERS - 1) * BASINS * LAYERS * (8 * LANES // NBANDS))
    s2[...] = total * (1.0 / norm)

    @pl.loop(1, PEERS)
    def _(i):
        remote(s2, piece(df, e), c3_s, c3_r, peer(i)[1]).start()

    piece(df, e)[...] = s2[...]

    for m in range(MINE):
        core_copy(m).wait_send()
        for c in x_copies(m).values():
            c().wait_send()
        wait_bytes(ys, (SPREAD - 1) * PAD, yz_s.at[m])
    means_over.wait_send()
    wait_bytes(c1, (PEERS - 1) * PAD, c1_s)
    wait_bytes(mm, (PEERS - 1) * 2 * PAD, m2_s)
    wait_bytes(c2, (SPREAD - 1) * PAD, c2_s)
    wait_bytes(df, (PEERS - 1) * PAD, c3_s)

    wait_bytes(df, (PEERS - 1) * PAD, c3_r)
    for c in range(NBANDS):
        rows = df[pl.ds(c, 8, stride=PAD), :]
        for q in range(4):
            part = rows if q == 0 else pltpu.roll(rows, LANES - MEMBERS * q, 1)
            cov_out[c, pl.ds(q * 8, 8), :] = part[:, :MEMBERS]


def lat_tiles(a):
    *lead, cols, lats = a.shape
    a = a.reshape(*lead, cols, lats // LANES, LANES)
    a = jnp.swapaxes(a, -3, -2)
    return a.reshape(-1, LANES)


def local(v, h, t, lab, zone):
    lats = v.shape[-1]
    columns = COLS * 16
    spacing = (metric_factor(lats) / math.sqrt(columns)).reshape(8, LANES)
    vmem = lambda *s: pltpu.VMEM(s, F32)
    big = MINE * LAYERS * COLS * 8
    dma = pltpu.SemaphoreType.DMA
    anywhere = pl.BlockSpec(memory_space=pl.ANY)
    inside = pl.BlockSpec(memory_space=pltpu.VMEM)
    psi, heat, cov = pl.pallas_call(
        kernel,
        out_shape=(
            jax.ShapeDtypeStruct((BASINS, LAYERS, 8), F32),
            jax.ShapeDtypeStruct((BASINS, 8), F32),
            jax.ShapeDtypeStruct((NBANDS, MEMBERS, MEMBERS), F32),
        ),
        in_specs=[anywhere] * 3 + [inside] * 3,
        out_specs=(inside, inside, inside),
        scratch_shapes=[
            vmem(big, LANES), vmem(big, LANES), vmem(big, LANES),
            vmem(COLS * BASINS, 8, LANES),
            vmem(COLS, 8, LANES),
            vmem(MINE, 2, LAYERS // 2, ROWS, 8, LANES),
            vmem(MINE, LAYERS // 2, ROWS, 8, LANES),
            vmem(MINE, LAYERS // 2, ROWS, 8, LANES),
            vmem(MINE, ROWS, 8, LANES),
            vmem(MINE, ROWS, 8, LANES),
            vmem(MINE, 2, ROWS, 8, LANES),
            vmem(MINE, 2, ROWS, 8, LANES),
            vmem(MINE, 2, ROWS, 8, LANES),
            vmem(MINE * SPREAD * PAD, LANES),
            vmem(MINE * SPREAD * PAD, LANES),
            vmem(BASINS * MEMBERS, LANES),
            vmem(MEMBERS * MEMBERS, LANES),
            vmem(PEERS * PAD, LANES),
            vmem(PEERS * PAD, LANES),
            vmem(PAD, LANES),
            vmem(SPREAD * PAD, LANES),
            vmem(PAD, LANES),
            vmem(PEERS * PAD, LANES),
            vmem(PAD, LANES),
            vmem(PEERS * 2 * PAD, LANES),
            dma((MINE, 3)),
            dma((MINE,)), dma((MINE,)),
            dma((MINE, 6)), dma((MINE, 6)),
            dma((MINE,)), dma((MINE,)),
            dma, dma, dma, dma, dma, dma, dma, dma, dma, dma,
        ],
        compiler_params=pltpu.CompilerParams(collective_id=0, has_side_effects=True),
        name="overturning",
    )(lat_tiles(v), lat_tiles(h), lat_tiles(t), lat_tiles(lab), zone.reshape(8, LANES), spacing)
    return psi, heat, cov


def solution(mesh):
    return jax.shard_map(
        local,
        mesh=mesh,
        in_specs=(
            P("member", None, "tile", None),
            P("member", None, "tile", None),
            P("member", None, "tile", None),
            P("tile", None),
            P(),
        ),
        out_specs=(
            P(None, None, ("member", "tile")),
            P(None, ("member", "tile")),
            P(),
        ),
        check_vma=False,
    )
```

```python
import math

import jax
import jax.numpy as jnp
from jax import lax
from jax.experimental import pallas as pl
from jax.experimental.pallas import tpu as pltpu
from jax.sharding import PartitionSpec as P

MESH = pl.DeviceIdType.MESH
F32 = jnp.float32
BF16 = jnp.bfloat16

LANES = 128
BASINS = 10
LAYERS = 16
NBANDS = 16
MEMBERS = 32
GROUPS = 8
MINE = MEMBERS // GROUPS
COLS = 8
ROWS = BASINS + 1
PAD = 16
RING = 4
PEERS = 8
SPREAD = 16


def metric_factor(row):
    lats = 8 * LANES
    index = lax.broadcasted_iota(jnp.int32, (8, LANES), 1) + row * LANES
    degrees = -80.0 + 160.0 * (index.astype(F32) + 0.5) / lats
    return jnp.cos(degrees * (math.pi / 180.0)) * (1.0 / math.sqrt(COLS * 16))


def kernel(
    v_hbm, h_hbm, t_hbm, lab_hbm, zone_hbm,
    psi_out, heat_out, cov_out,
    vb, hb, tb, lab_ref, zone_ref, onehot, heat_cols, ps, cr, xs, fa, fb, na, nb, rl, ys, rb,
    an, pp, dd, c1, s1, c2, s2, df, mb, mm,
    hbm_sem, small_sem, core_s, core_r, x_s, x_r, yz_s, yz_r,
    c1_s, c1_r, c2_s, c2_r, c3_s, c3_r, m1_s, m1_r, m2_s, m2_r,
):
    member = lax.axis_index("member")
    tile = lax.axis_index("tile")
    z_hi = tile // PEERS
    e = tile % PEERS
    x = e // 2
    core = e % 2
    me = z_hi * GROUPS + member

    def peer(i):
        other = lax.rem(e + i, PEERS)
        return other, {"member": member, "tile": z_hi * PEERS + other}

    def spread(i):
        other = lax.rem(me + i, SPREAD)
        return other, {"member": other % GROUPS, "tile": (other // GROUPS) * PEERS + e}

    def along_x(step):
        other = lax.rem(x + RING + step, RING)
        return {"member": member, "tile": z_hi * PEERS + other * 2 + core}

    sibling = {"member": member, "tile": z_hi * PEERS + x * 2 + (1 - core)}

    def remote(src, dst, send, recv, device):
        return pltpu.make_async_remote_copy(
            src_ref=src, dst_ref=dst, send_sem=send, recv_sem=recv,
            device_id=device, device_id_type=MESH,
        )

    chunk = LAYERS * COLS * 8

    def load(m):
        rows = pl.ds(m * chunk, chunk)
        return [
            pltpu.make_async_copy(a.at[rows], b.at[rows], hbm_sem.at[m, i])
            for i, (a, b) in enumerate(((v_hbm, vb), (h_hbm, hb), (t_hbm, tb)))
        ]

    labels = pltpu.make_async_copy(lab_hbm, lab_ref, small_sem.at[0])
    zones = pltpu.make_async_copy(zone_hbm, zone_ref, small_sem.at[1])
    labels.start()
    for m in range(2):
        for c in load(m):
            c.start()
    zones.start()

    barrier = pltpu.get_barrier_semaphore()

    @pl.loop(1, PEERS)
    def _(i):
        pl.semaphore_signal(barrier, inc=1, device_id=peer(i)[1], device_id_type=MESH)

    @pl.loop(1, SPREAD)
    def _(i):
        pl.semaphore_signal(barrier, inc=1, device_id=spread(i)[1], device_id_type=MESH)

    labels.wait()
    for col in range(COLS):
        lab = lab_ref[pl.ds(col, 8, stride=8), :]
        for b in range(BASINS):
            onehot[col * BASINS + b] = jnp.where(lab == b, 1.0, 0.0).astype(F32)
    zero = jnp.zeros((8, LANES), F32)
    for col in range(COLS):
        heat_cols[col] = zero

    def rows_of(m):
        return ROWS if m == MINE - 1 else BASINS

    def compute(m):
        with jax.named_scope("hbm_wait"):
            for c in load(m):
                c.wait()
        if m + 2 < MINE:
            for c in load(m + 2):
                c.start()

        def body(kk, carry):
            acc, hs = list(carry[0]), list(carry[1])
            nxt = [None] * BASINS
            for col in range(COLS):
                base = m * chunk + kk * (2 * COLS * 8) + col
                first = pl.ds(base, 8, stride=8)
                second = pl.ds(base + COLS * 8, 8, stride=8)
                u0 = vb[first, :] * hb[first, :]
                u1 = vb[second, :] * hb[second, :]
                hs[col] = hs[col] + (u0 * tb[first, :] + u1 * tb[second, :])
                for b in range(BASINS):
                    o = onehot[col * BASINS + b]
                    acc[b] = acc[b] + o * u0
                    nxt[b] = o * u1 if nxt[b] is None else nxt[b] + o * u1
            for b in range(BASINS):
                ps[m, 0, kk, b] = acc[b]
                acc[b] = acc[b] + nxt[b]
                ps[m, 1, kk, b] = acc[b]
            return tuple(acc), tuple(hs)

        start = (tuple(zero for _ in range(BASINS)), tuple(heat_cols[c] for c in range(COLS)))
        with jax.named_scope("zonal"):
            _, hs = lax.fori_loop(0, LAYERS // 2, body, start)
        if m < MINE - 1:
            for col in range(COLS):
                heat_cols[col] = hs[col]
        else:
            for k in range(LAYERS):
                row = zero
                if k < BASINS:
                    for col in range(COLS):
                        row = row + onehot[col * BASINS + k] * hs[col]
                ps[m, k % 2, k // 2, BASINS] = row

    def core_copy(m):
        n = rows_of(m)
        return remote(
            ps.at[m, 1 - core, :, pl.ds(0, n)], cr.at[m, :, pl.ds(0, n)],
            core_s.at[m], core_r.at[m], sibling,
        )

    right, left = along_x(1), along_x(-1)
    at_right = lax.rem(x + 1, RING)
    at_left = lax.rem(x + 3, RING)
    at_far = lax.rem(x + 2, RING)

    def x_copies(m):
        n = pl.ds(0, rows_of(m))
        hi = RING

        def c(i, src, dst, device):
            return lambda: remote(src, dst, x_s.at[m, i], x_r.at[m, i], device)

        return dict(
            far_right=c(0, xs.at[m, at_far, n], fa.at[m, n], right),
            far_left=c(1, xs.at[m, hi + at_far, n], fb.at[m, n], left),
            near_right=c(2, xs.at[m, hi + at_right, n], na.at[m, 1, n], right),
            near_left=c(3, xs.at[m, at_left, n], nb.at[m, 0, n], left),
            sum_right=c(4, rl.at[m, 0, n], na.at[m, 0, n], right),
            sum_left=c(5, rl.at[m, 1, n], nb.at[m, 1, n], left),
        )

    def pair_sum(m):
        with jax.named_scope("core_wait"):
            core_copy(m).wait_recv()
        n = rows_of(m)

        def one(kk, _):
            for r in range(n):
                xs[m, kk, r] = ps[m, core, kk, r] + cr[m, kk, r]
            return 0

        copies = x_copies(m)
        with jax.named_scope("pair_sum"):
            lax.fori_loop(0, LAYERS // 2, one, 0)
        for name in ("far_right", "far_left", "near_right", "near_left"):
            copies[name]().start()

    def relay(m):
        copies = x_copies(m)
        n = rows_of(m)
        with jax.named_scope("far_wait"):
            copies["far_right"]().wait_recv()
        for r in range(n):
            rl[m, 0, r] = xs[m, at_right, r] + fa[m, r]
        copies["sum_right"]().start()
        with jax.named_scope("far_wait"):
            copies["far_left"]().wait_recv()
        for r in range(n):
            rl[m, 1, r] = xs[m, RING + at_left, r] + fb[m, r]
        copies["sum_left"]().start()

    def piece(ref, i):
        return ref.at[pl.ds(pl.multiple_of(i * PAD, PAD), PAD)]

    def spread_out(m):
        copies = x_copies(m)
        n = rows_of(m)
        with jax.named_scope("near_wait"):
            for name in ("near_right", "near_left", "sum_right", "sum_left"):
                copies[name]().wait_recv()
        for z in range(2):
            for r in range(n):
                total = xs[m, z * RING + x, r] + (na[m, z, r] + nb[m, z, r])
                ys[pl.ds((m * SPREAD + z * GROUPS) * PAD + r, 8, stride=PAD), :] = total
        for r in range(n, PAD):
            for z in range(2):
                ys[pl.ds((m * SPREAD + z * GROUPS) * PAD + r, 8, stride=PAD), :] = zero

        @pl.loop(1, SPREAD)
        def _(i):
            other, device = spread(i)
            remote(
                piece(ys, m * SPREAD + other), piece(rb, me * MINE + m),
                yz_s.at[m], yz_r.at[m], device,
            ).start()

        piece(rb, me * MINE + m)[...] = piece(ys, m * SPREAD + me)[...]

    def wait_bytes(ref, rows, sem):
        view = ref.at[pl.ds(0, rows)]
        pltpu.make_async_copy(view, view, sem).wait()

    spacing = metric_factor(member)

    compute(0)
    with jax.named_scope("entry"):
        pl.semaphore_wait(barrier, PEERS - 1 + SPREAD - 1)
    core_copy(0).start()
    compute(1)
    core_copy(1).start()
    pair_sum(0)
    compute(2)
    core_copy(2).start()
    pair_sum(1)
    relay(0)
    compute(3)
    core_copy(3).start()
    pair_sum(2)
    relay(1)
    pair_sum(3)
    spread_out(0)
    relay(2)
    spread_out(1)
    relay(3)
    spread_out(2)
    spread_out(3)
    with jax.named_scope("yz_wait"):
        for m in range(MINE):
            wait_bytes(ys, (SPREAD - 1) * PAD, yz_r.at[m])

    with jax.named_scope("anomaly"):
        for b in range(BASINS):
            a = []
            for q in range(4):
                lo = rb[pl.ds(q * 8 * PAD + b, 8, stride=PAD), :]
                hi = rb[pl.ds((MEMBERS + q * 8) * PAD + b, 8, stride=PAD), :]
                a.append((lo + hi) * spacing)
            mean = jnp.sum((a[0] + a[1]) + (a[2] + a[3]), axis=0, keepdims=True) * (1.0 / MEMBERS)
            mb[pl.ds(b, 1), :] = mean
            for q in range(4):
                an[pl.ds(b * MEMBERS + q * 8, 8), :] = a[q] - mean
        last = (MINE - 1) * PAD + BASINS
        warm = rb[pl.ds(last, 8, stride=MINE * PAD), :] + rb[
            pl.ds(last + GROUPS * MINE * PAD, 8, stride=MINE * PAD), :
        ]
        warm = jnp.sum(warm * spacing, axis=0, keepdims=True)
        mb[pl.ds(BASINS, 1), :] = warm * (1.0 / (MEMBERS * math.sqrt(LAYERS)))
        for r in range(ROWS, PAD):
            mb[pl.ds(r, 1), :] = jnp.zeros((1, LANES), F32)

    mm[pl.ds(pl.multiple_of((e * 2 + z_hi) * PAD, PAD), PAD), :] = mb[...]
    means_over = remote(
        mb, piece(mm, e * 2 + z_hi), m1_s, m1_r,
        {"member": member, "tile": (1 - z_hi) * PEERS + e},
    )
    means_over.start()

    def gram(n, _):
        acc = [None] * 4
        for b in range(BASINS):
            row = jnp.broadcast_to(an[pl.ds(b * MEMBERS + n, 1), :], (8, LANES))
            for q in range(4):
                t = row * an[pl.ds(b * MEMBERS + q * 8, 8), :]
                acc[q] = t if acc[q] is None else acc[q] + t
        at = pl.multiple_of((n % 8) * LANES + (n // 8) * MEMBERS, MEMBERS)
        for q in range(4):
            pp[pl.ds(at + q * 8, 8), :] = acc[q]
        return 0

    with jax.named_scope("gram"):
        lax.fori_loop(0, MEMBERS, gram, 0)

    zones.wait()
    zone = jnp.broadcast_to(zone_ref[pl.ds(member, 1), :], (NBANDS, LANES))
    band = jnp.where(
        zone == lax.broadcasted_iota(jnp.int32, (NBANDS, LANES), 0), 1.0, 0.0
    ).astype(BF16)
    with jax.named_scope("band"):
        for r in range(8):
            p = pp[pl.ds(r * LANES, LANES), :]
            total = None
            for _ in range(3):
                part = p.astype(BF16)
                p = p - part.astype(F32)
                d = lax.dot_general(
                    band, part, (((1,), (1,)), ((), ())), preferred_element_type=F32
                )
                total = d if total is None else total + d
            dd[pl.ds(r * PAD, PAD), :] = total

    @pl.loop(1, PEERS)
    def _(i):
        other, device = peer(i)
        remote(piece(dd, other), piece(c1, e), c1_s, c1_r, device).start()

    piece(c1, e)[...] = piece(dd, e)[...]
    with jax.named_scope("c1_wait"):
        wait_bytes(c1, (PEERS - 1) * PAD, c1_r)
    total = c1[pl.ds(0, PAD), :]
    for i in range(1, PEERS):
        total = total + c1[pl.ds(i * PAD, PAD), :]
    s1[...] = total

    @pl.loop(1, SPREAD)
    def _(i):
        remote(s1, piece(c2, me), c2_s, c2_r, spread(i)[1]).start()

    piece(c2, me)[...] = total

    with jax.named_scope("mean_wait"):
        means_over.wait_recv()
    both = pl.ds(pl.multiple_of(e * 2 * PAD, PAD), 2 * PAD)

    @pl.loop(1, PEERS)
    def _(i):
        remote(mm.at[both], mm.at[both], m2_s, m2_r, peer(i)[1]).start()

    with jax.named_scope("c2_wait"):
        wait_bytes(c2, (SPREAD - 1) * PAD, c2_r)
    total = c2[pl.ds(0, PAD), :]
    for i in range(1, SPREAD):
        total = total + c2[pl.ds(i * PAD, PAD), :]
    norm = float((MEMBERS - 1) * BASINS * LAYERS * (8 * LANES // NBANDS))
    s2[...] = total * (1.0 / norm)

    @pl.loop(1, PEERS)
    def _(i):
        remote(s2, piece(df, e), c3_s, c3_r, peer(i)[1]).start()

    piece(df, e)[...] = s2[...]

    with jax.named_scope("mm_wait"):
        wait_bytes(mm, (PEERS - 1) * 2 * PAD, m2_r)
    turn = lax.rem(LANES - tile * 8, LANES)
    with jax.named_scope("mean_out"):
        for b in range(BASINS):
            rows = [mm[pl.ds(z * PAD + b, 8, stride=2 * PAD), :] for z in range(2)]
            rows = pltpu.roll(jnp.concatenate(rows, axis=0), turn, 1)
            psi_out[b] = jnp.swapaxes(rows, 0, 1)[:8, :]
        rows = [mm[pl.ds(z * PAD + BASINS, 8, stride=2 * PAD), :] for z in range(2)]
        rows = pltpu.roll(jnp.concatenate(rows, axis=0), turn, 1)
        heat_out[...] = jnp.swapaxes(rows, 0, 1)[:8, :BASINS]

    with jax.named_scope("send_wait"):
        for m in range(MINE):
            core_copy(m).wait_send()
            for c in x_copies(m).values():
                c().wait_send()
            wait_bytes(ys, (SPREAD - 1) * PAD, yz_s.at[m])
        means_over.wait_send()
        wait_bytes(c1, (PEERS - 1) * PAD, c1_s)
        wait_bytes(mm, (PEERS - 1) * 2 * PAD, m2_s)
        wait_bytes(c2, (SPREAD - 1) * PAD, c2_s)
        wait_bytes(df, (PEERS - 1) * PAD, c3_s)

    with jax.named_scope("c3_wait"):
        wait_bytes(df, (PEERS - 1) * PAD, c3_r)
    for c in range(NBANDS):
        rows = df[pl.ds(c, 8, stride=PAD), :]
        for q in range(4):
            part = rows if q == 0 else pltpu.roll(rows, LANES - MEMBERS * q, 1)
            cov_out[c, pl.ds(q * 8, 8), :] = part[:, :MEMBERS]


def lat_tiles(a):
    *lead, cols, lats = a.shape
    a = a.reshape(*lead, cols, lats // LANES, LANES)
    a = jnp.swapaxes(a, -3, -2)
    return a.reshape(-1, LANES)


def finish(psi, heat, cov, psi_out, heat_out, cov_out, sem):
    copies = [
        pltpu.make_async_copy(a, b, sem.at[i])
        for i, (a, b) in enumerate(((psi, psi_out), (heat, heat_out), (cov, cov_out)))
    ]
    for c in copies:
        c.start()
    for c in copies:
        c.wait()


def local(v, h, t, lab, zone):
    vmem = lambda *s: pltpu.VMEM(s, F32)
    big = MINE * LAYERS * COLS * 8
    dma = pltpu.SemaphoreType.DMA
    anywhere = pl.BlockSpec(memory_space=pl.ANY)
    inside = pl.BlockSpec(memory_space=pltpu.VMEM)
    shapes = ((BASINS, 8, LAYERS), (8, BASINS), (NBANDS, MEMBERS, MEMBERS))
    outs = pl.pallas_call(
        kernel,
        out_shape=tuple(pltpu.VMEM(s, F32) for s in shapes),
        in_specs=[anywhere] * 5,
        out_specs=(inside, inside, inside),
        scratch_shapes=[
            vmem(big, LANES), vmem(big, LANES), vmem(big, LANES),
            pltpu.VMEM((COLS * 8, LANES), jnp.int32),
            pltpu.VMEM((8, LANES), jnp.int32),
            vmem(COLS * BASINS, 8, LANES),
            vmem(COLS, 8, LANES),
            vmem(MINE, 2, LAYERS // 2, ROWS, 8, LANES),
            vmem(MINE, LAYERS // 2, ROWS, 8, LANES),
            vmem(MINE, LAYERS // 2, ROWS, 8, LANES),
            vmem(MINE, ROWS, 8, LANES),
            vmem(MINE, ROWS, 8, LANES),
            vmem(MINE, 2, ROWS, 8, LANES),
            vmem(MINE, 2, ROWS, 8, LANES),
            vmem(MINE, 2, ROWS, 8, LANES),
            vmem(MINE * SPREAD * PAD, LANES),
            vmem(MINE * SPREAD * PAD, LANES),
            vmem(BASINS * MEMBERS, LANES),
            vmem(MEMBERS * MEMBERS, LANES),
            vmem(PEERS * PAD, LANES),
            vmem(PEERS * PAD, LANES),
            vmem(PAD, LANES),
            vmem(SPREAD * PAD, LANES),
            vmem(PAD, LANES),
            vmem(PEERS * PAD, LANES),
            vmem(PAD, LANES),
            vmem(PEERS * 2 * PAD, LANES),
            dma((MINE, 3)), dma((2,)),
            dma((MINE,)), dma((MINE,)),
            dma((MINE, 6)), dma((MINE, 6)),
            dma((MINE,)), dma((MINE,)),
            dma, dma, dma, dma, dma, dma, dma, dma, dma, dma,
        ],
        compiler_params=pltpu.CompilerParams(
            collective_id=0, has_side_effects=True, vmem_limit_bytes=60 << 20
        ),
        name="overturning",
    )(lat_tiles(v), lat_tiles(h), lat_tiles(t), lat_tiles(lab), zone.reshape(8, LANES))
    psi, heat, cov = pl.pallas_call(
        finish,
        out_shape=tuple(jax.ShapeDtypeStruct(s, F32) for s in shapes),
        in_specs=[inside] * 3,
        out_specs=(anywhere,) * 3,
        scratch_shapes=[dma((3,))],
        compiler_params=pltpu.CompilerParams(vmem_limit_bytes=1 << 20),
        name="finish",
    )(*outs)
    return jnp.swapaxes(psi, 1, 2), jnp.swapaxes(heat, 0, 1), cov


def solution(mesh):
    return jax.shard_map(
        local,
        mesh=mesh,
        in_specs=(
            P("member", None, "tile", None),
            P("member", None, "tile", None),
            P("member", None, "tile", None),
            P("tile", None),
            P(),
        ),
        out_specs=(
            P(None, None, ("member", "tile")),
            P(None, ("member", "tile")),
            P(),
        ),
        check_vma=False,
    )
```

```python
import math

import jax
import jax.numpy as jnp
from jax import lax
from jax.experimental import pallas as pl
from jax.experimental.pallas import tpu as pltpu
from jax.sharding import PartitionSpec as P

MESH = pl.DeviceIdType.MESH
F32 = jnp.float32
BF16 = jnp.bfloat16

LANES = 128
BASINS = 10
LAYERS = 16
NBANDS = 16
MEMBERS = 32
GROUPS = 8
MINE = MEMBERS // GROUPS
COLS = 8
ROWS = BASINS + 1
PAD = 16
RING = 4
PEERS = 8
SPREAD = 16
TURNED = (1,)
WIDE = RING * BASINS
FAR_PEERS = (4, 3, 5, 2, 6, 1, 7)
FAR_SPREAD = (12, 4, 13, 11, 5, 3, 14, 10, 6, 2, 8, 15, 9, 7, 1)


def metric_factor(row):
    lats = 8 * LANES
    index = lax.broadcasted_iota(jnp.int32, (8, LANES), 1) + row * LANES
    degrees = -80.0 + 160.0 * (index.astype(F32) + 0.5) / lats
    return jnp.cos(degrees * (math.pi / 180.0)) * (1.0 / math.sqrt(COLS * 16))


def kernel(
    v_hbm, h_hbm, t_hbm, lab_hbm, zone_hbm,
    psi_out, heat_out, cov_out,
    vb, hb, tb, lab_ref, zone_ref, onehot, heat_cols, ps, cr, xs, fa, fb, na, nb, rl,
    ys, rb, yf, rf, an, dd, c1, s1, c2, s2, df, mb, mm,
    hbm_sem, small_sem, core_s, core_r, x_s, x_r, yz_s, yz_r,
    c_s, c1_r, c2_r, c3_r, m1_r, m2_r,
):
    member = lax.axis_index("member")
    tile = lax.axis_index("tile")
    z_hi = tile // PEERS
    e = tile % PEERS
    x = e // 2
    core = e % 2
    me = z_hi * GROUPS + member

    def peer(i):
        other = lax.rem(e + i, PEERS)
        return other, {"member": member, "tile": z_hi * PEERS + other}

    def spread(i):
        other = lax.rem(me + i, SPREAD)
        return other, {"member": other % GROUPS, "tile": (other // GROUPS) * PEERS + e}

    def along_x(step):
        other = lax.rem(x + RING + step, RING)
        return {"member": member, "tile": z_hi * PEERS + other * 2 + core}

    sibling = {"member": member, "tile": z_hi * PEERS + x * 2 + (1 - core)}

    def remote(src, dst, send, recv, device):
        return pltpu.make_async_remote_copy(
            src_ref=src, dst_ref=dst, send_sem=send, recv_sem=recv,
            device_id=device, device_id_type=MESH,
        )

    def wait_bytes(ref, rows, sem):
        view = ref.at[pl.ds(0, rows)]
        pltpu.make_async_copy(view, view, sem).wait()

    chunk = LAYERS * COLS * 8

    def load(m):
        rows = pl.ds(m * chunk, chunk)
        return [
            pltpu.make_async_copy(a.at[rows], b.at[rows], hbm_sem.at[m])
            for a, b in ((v_hbm, vb), (h_hbm, hb), (t_hbm, tb))
        ]

    labels = pltpu.make_async_copy(lab_hbm, lab_ref, small_sem.at[0])
    zones = pltpu.make_async_copy(zone_hbm, zone_ref, small_sem.at[1])
    labels.start()
    for m in range(2):
        for c in load(m):
            c.start()
    zones.start()

    barrier = pltpu.get_barrier_semaphore()

    @pl.loop(1, PEERS)
    def _(i):
        pl.semaphore_signal(barrier, inc=1, device_id=peer(i)[1], device_id_type=MESH)

    @pl.loop(1, SPREAD)
    def _(i):
        pl.semaphore_signal(barrier, inc=1, device_id=spread(i)[1], device_id_type=MESH)

    labels.wait()
    for col in range(COLS):
        lab = lab_ref[pl.ds(col, 8, stride=8), :]
        for b in range(BASINS):
            onehot[col * BASINS + b] = jnp.where(lab == b, 1.0, 0.0).astype(F32)
    zero = jnp.zeros((8, LANES), F32)
    for col in range(COLS):
        heat_cols[col] = zero

    def rows_of(m):
        return ROWS if m == MINE - 1 else BASINS

    def half_of(m):
        return BASINS // 2 if m in TURNED else rows_of(m)

    def compute(m):
        with jax.named_scope("hbm_wait"):
            wait_bytes(vb, 3 * chunk, hbm_sem.at[m])
        if m + 2 < MINE:
            for c in load(m + 2):
                c.start()

        def body(kk, carry):
            acc, hs = list(carry[0]), list(carry[1])
            nxt = [None] * BASINS
            for col in range(COLS):
                base = m * chunk + kk * (2 * COLS * 8) + col
                first = pl.ds(base, 8, stride=8)
                second = pl.ds(base + COLS * 8, 8, stride=8)
                u0 = vb[first, :] * hb[first, :]
                u1 = vb[second, :] * hb[second, :]
                hs[col] = hs[col] + (u0 * tb[first, :] + u1 * tb[second, :])
                for b in range(BASINS):
                    o = onehot[col * BASINS + b]
                    acc[b] = acc[b] + o * u0
                    nxt[b] = o * u1 if nxt[b] is None else nxt[b] + o * u1
            for b in range(BASINS):
                ps[m, 0, kk, b] = acc[b]
                acc[b] = acc[b] + nxt[b]
                ps[m, 1, kk, b] = acc[b]
            return tuple(acc), tuple(hs)

        start = (tuple(zero for _ in range(BASINS)), tuple(heat_cols[c] for c in range(COLS)))
        with jax.named_scope("zonal"):
            _, hs = lax.fori_loop(0, LAYERS // 2, body, start)
        if m < MINE - 1:
            for col in range(COLS):
                heat_cols[col] = hs[col]
        else:
            for k in range(LAYERS):
                row = zero
                if k < BASINS:
                    for col in range(COLS):
                        row = row + onehot[col * BASINS + k] * hs[col]
                ps[m, k % 2, k // 2, BASINS] = row

    def core_copy(m):
        n = rows_of(m)
        return remote(
            ps.at[m, 1 - core, :, pl.ds(0, n)], cr.at[m, :, pl.ds(0, n)],
            core_s, core_r.at[m], sibling,
        )

    right, left = along_x(1), along_x(-1)
    at_right = lax.rem(x + 1, RING)
    at_left = lax.rem(x + 3, RING)
    at_far = lax.rem(x + 2, RING)

    def x_copies(m):
        n = pl.ds(0, half_of(m))
        hi = RING

        def c(i, src, dst, device):
            return lambda: remote(src, dst, x_s, x_r.at[m, i], device)

        return dict(
            far_right=c(0, xs.at[m, at_far, n], fa.at[m, n], right),
            far_left=c(1, xs.at[m, hi + at_far, n], fb.at[m, n], left),
            near_right=c(2, xs.at[m, hi + at_right, n], na.at[m, 1, n], right),
            near_left=c(2, xs.at[m, at_left, n], nb.at[m, 0, n], left),
            sum_right=c(2, rl.at[m, 0, n], na.at[m, 0, n], right),
            sum_left=c(2, rl.at[m, 1, n], nb.at[m, 1, n], left),
        )

    def start_x(m):
        copies = x_copies(m)
        for name in ("far_right", "far_left", "near_right", "near_left"):
            copies[name]().start()

    def near_wait(m):
        with jax.named_scope("near_wait"):
            wait_bytes(vb, 4 * half_of(m) * 8, x_r.at[m, 2])

    def pair_sum(m):
        with jax.named_scope("core_wait"):
            core_copy(m).wait_recv()
        n = rows_of(m)

        def one(kk, _):
            for r in range(n):
                xs[m, kk, r] = ps[m, core, kk, r] + cr[m, kk, r]
            return 0

        with jax.named_scope("pair_sum"):
            lax.fori_loop(0, LAYERS // 2, one, 0)
        start_x(m)

    def relay(m):
        copies = x_copies(m)
        n = half_of(m)
        with jax.named_scope("far_wait"):
            copies["far_right"]().wait_recv()
        for r in range(n):
            rl[m, 0, r] = xs[m, at_right, r] + fa[m, r]
        copies["sum_right"]().start()
        with jax.named_scope("far_wait"):
            copies["far_left"]().wait_recv()
        for r in range(n):
            rl[m, 1, r] = xs[m, RING + at_left, r] + fb[m, r]
        copies["sum_left"]().start()

    def piece(ref, i, rows=PAD):
        return ref.at[pl.ds(pl.multiple_of(i * rows, 8), rows)]

    def spread_out(m):
        n = rows_of(m)
        near_wait(m)
        for z in range(2):
            for r in range(n):
                total = xs[m, z * RING + x, r] + (na[m, z, r] + nb[m, z, r])
                ys[pl.ds((m * SPREAD + z * GROUPS) * PAD + r, 8, stride=PAD), :] = total
        for i in FAR_SPREAD:
            other, device = spread(i)
            remote(
                piece(ys, m * SPREAD + other), piece(rb, me * MINE + m),
                yz_s, yz_r.at[m], device,
            ).start()
        piece(rb, me * MINE + m)[...] = piece(ys, m * SPREAD + me)[...]

    def turn_out(m):
        with jax.named_scope("core_wait"):
            core_copy(m).wait_recv()
        base = TURNED.index(m) * SPREAD

        def one(kk, _):
            at = (base + lax.div(kk, RING) * GROUPS) * WIDE + lax.rem(kk, RING) * BASINS
            for r in range(BASINS):
                total = ps[m, core, kk, r] + cr[m, kk, r]
                yf[pl.ds(at + r, 8, stride=WIDE), :] = total
            return 0

        with jax.named_scope("turn_sum"):
            lax.fori_loop(0, LAYERS // 2, one, 0)
        for i in FAR_SPREAD:
            other, device = spread(i)
            remote(
                piece(yf, base + other, WIDE), piece(rf, base + me, WIDE),
                yz_s, yz_r.at[m], device,
            ).start()
        piece(rf, base + me, WIDE)[...] = piece(yf, base + me, WIDE)[...]

    def turn_in(m):
        with jax.named_scope("turn_wait"):
            wait_bytes(vb, (SPREAD - 1) * WIDE, yz_r.at[m])
        base = TURNED.index(m) * SPREAD * WIDE
        for k in range(RING):
            for b in range(BASINS):
                at = base + k * BASINS + b
                half, r = divmod(b, BASINS // 2)
                xs[m, half * RING + k, r] = (
                    rf[pl.ds(at, 8, stride=WIDE), :]
                    + rf[pl.ds(at + GROUPS * WIDE, 8, stride=WIDE), :]
                )
        start_x(m)

    def turn_end(m):
        near_wait(m)
        for b in range(BASINS):
            half, r = divmod(b, BASINS // 2)
            total = xs[m, half * RING + x, r] + (na[m, half, r] + nb[m, half, r])
            rb[pl.ds(m * PAD + b, 8, stride=MINE * PAD), :] = total

    spacing = metric_factor(member)

    for m in TURNED:
        for b in range(BASINS):
            rb[pl.ds((MEMBERS + m) * PAD + b, 8, stride=MINE * PAD), :] = zero

    compute(0)
    with jax.named_scope("entry"):
        pl.semaphore_wait(barrier, PEERS - 1 + SPREAD - 1)
    core_copy(0).start()
    compute(1)
    core_copy(1).start()
    pair_sum(0)
    compute(2)
    core_copy(2).start()
    turn_out(1)
    pair_sum(2)
    compute(3)
    core_copy(3).start()
    relay(0)
    pair_sum(3)
    relay(2)
    spread_out(0)
    turn_in(1)
    relay(3)
    spread_out(2)
    relay(1)
    spread_out(3)
    turn_end(1)
    with jax.named_scope("yz_wait"):
        for m in range(MINE):
            if m not in TURNED:
                wait_bytes(vb, (SPREAD - 1) * PAD, yz_r.at[m])

        for b in range(BASINS):
            a = []
            for q in range(4):
                lo = rb[pl.ds(q * 8 * PAD + b, 8, stride=PAD), :]
                hi = rb[pl.ds((MEMBERS + q * 8) * PAD + b, 8, stride=PAD), :]
                a.append((lo + hi) * spacing)
            mean = jnp.sum((a[0] + a[1]) + (a[2] + a[3]), axis=0, keepdims=True) * (1.0 / MEMBERS)
            mb[pl.ds(b, 1), :] = mean
            for q in range(4):
                an[pl.ds(b * MEMBERS + q * 8, 8), :] = a[q] - mean
        last = (MINE - 1) * PAD + BASINS
        warm = rb[pl.ds(last, 8, stride=MINE * PAD), :] + rb[
            pl.ds(last + GROUPS * MINE * PAD, 8, stride=MINE * PAD), :
        ]
        warm = jnp.sum(warm * spacing, axis=0, keepdims=True)
        mb[pl.ds(BASINS, 1), :] = warm * (1.0 / (MEMBERS * math.sqrt(LAYERS)))
        for r in range(ROWS, PAD):
            mb[pl.ds(r, 1), :] = jnp.zeros((1, LANES), F32)

    mm[pl.ds(pl.multiple_of((e * 2 + z_hi) * PAD, PAD), PAD), :] = mb[...]
    means_over = remote(
        mb, piece(mm, e * 2 + z_hi), c_s, m1_r,
        {"member": member, "tile": (1 - z_hi) * PEERS + e},
    )
    means_over.start()

    zones.wait()
    zone = jnp.broadcast_to(zone_ref[pl.ds(member, 1), :], (NBANDS, LANES))
    band = jnp.where(
        zone == lax.broadcasted_iota(jnp.int32, (NBANDS, LANES), 0), 1.0, 0.0
    ).astype(BF16)
    band = jnp.concatenate([band] * 3, axis=1)

    @pl.loop(0, PEERS)
    def _(t):
        step = lax.div(t + 1, 2)
        i = PEERS // 2 + step * (1 - 2 * lax.rem(t, 2))
        other, device = peer(i)
        acc = [[None] * 4 for _ in range(4)]
        for b in range(BASINS):
            a = [an[pl.ds(b * MEMBERS + q * 8, 8), :] for q in range(4)]
            for k in range(4):
                row = an[pl.ds(b * MEMBERS + k * 8 + other, 1), :]
                row = jnp.broadcast_to(row, (8, LANES))
                for q in range(4):
                    p = row * a[q]
                    acc[k][q] = p if acc[k][q] is None else acc[k][q] + p
        p = jnp.concatenate([v for row in acc for v in row], axis=0)
        parts = []
        for _ in range(3):
            parts.append(p.astype(BF16))
            p = p - parts[-1].astype(F32)
        d = lax.dot_general(
            band, jnp.concatenate(parts, axis=1), (((1,), (1,)), ((), ())),
            preferred_element_type=F32,
        )
        piece(dd, other)[...] = d

        @pl.when(t < PEERS - 1)
        def _():
            remote(piece(dd, other), piece(c1, e), c_s, c1_r, device).start()

    piece(c1, e)[...] = piece(dd, e)[...]
    with jax.named_scope("c1_wait"):
        wait_bytes(c1, (PEERS - 1) * PAD, c1_r)
    total = c1[pl.ds(0, PAD), :]
    for i in range(1, PEERS):
        total = total + c1[pl.ds(i * PAD, PAD), :]
    s1[...] = total

    for i in FAR_SPREAD:
        remote(s1, piece(c2, me), c_s, c2_r, spread(i)[1]).start()

    piece(c2, me)[...] = total

    with jax.named_scope("mean_wait"):
        means_over.wait_recv()
    both = pl.ds(pl.multiple_of(e * 2 * PAD, PAD), 2 * PAD)

    for i in FAR_PEERS:
        remote(mm.at[both], mm.at[both], c_s, m2_r, peer(i)[1]).start()

    with jax.named_scope("c2_wait"):
        wait_bytes(c2, (SPREAD - 1) * PAD, c2_r)
    total = c2[pl.ds(0, PAD), :]
    for i in range(1, SPREAD):
        total = total + c2[pl.ds(i * PAD, PAD), :]
    norm = float((MEMBERS - 1) * BASINS * LAYERS * (8 * LANES // NBANDS))
    s2[...] = total * (1.0 / norm)

    for i in FAR_PEERS:
        remote(s2, piece(df, e), c_s, c3_r, peer(i)[1]).start()

    piece(df, e)[...] = s2[...]

    with jax.named_scope("mm_wait"):
        wait_bytes(mm, (PEERS - 1) * 2 * PAD, m2_r)
    turn = lax.rem(LANES - tile * 8, LANES)
    with jax.named_scope("mean_out"):
        for b in range(BASINS):
            rows = [mm[pl.ds(z * PAD + b, 8, stride=2 * PAD), :] for z in range(2)]
            rows = pltpu.roll(jnp.concatenate(rows, axis=0), turn, 1)
            psi_out[b] = jnp.swapaxes(rows, 0, 1)[:8, :]
        rows = [mm[pl.ds(z * PAD + BASINS, 8, stride=2 * PAD), :] for z in range(2)]
        rows = pltpu.roll(jnp.concatenate(rows, axis=0), turn, 1)
        heat_out[...] = jnp.swapaxes(rows, 0, 1)[:8, :BASINS]

    with jax.named_scope("send_wait"):
        straight = [m for m in range(MINE) if m not in TURNED]
        wait_bytes(vb, 8 * sum(rows_of(m) for m in range(MINE)) * LAYERS // 2, core_s)
        wait_bytes(vb, 8 * 6 * sum(half_of(m) for m in range(MINE)), x_s)
        wait_bytes(vb, (SPREAD - 1) * (len(straight) * PAD + len(TURNED) * WIDE), yz_s)
        wait_bytes(vb, ((PEERS - 1) * 4 + SPREAD) * PAD, c_s)

    with jax.named_scope("c3_wait"):
        wait_bytes(df, (PEERS - 1) * PAD, c3_r)
    for c in range(NBANDS):
        rows = df[pl.ds(c, 8, stride=PAD), :]
        for q in range(4):
            part = rows if q == 0 else pltpu.roll(rows, LANES - MEMBERS * q, 1)
            cov_out[c, pl.ds(q * 8, 8), :] = part[:, :MEMBERS]


def lat_tiles(a):
    *lead, cols, lats = a.shape
    a = a.reshape(*lead, cols, lats // LANES, LANES)
    a = jnp.swapaxes(a, -3, -2)
    return a.reshape(-1, LANES)


def finish(psi, heat, cov, psi_out, heat_out, cov_out, sem):
    copies = [
        pltpu.make_async_copy(a, b, sem.at[i])
        for i, (a, b) in enumerate(((psi, psi_out), (heat, heat_out), (cov, cov_out)))
    ]
    for c in copies:
        c.start()
    for c in copies:
        c.wait()


def local(v, h, t, lab, zone):
    vmem = lambda *s: pltpu.VMEM(s, F32)
    big = MINE * LAYERS * COLS * 8
    dma = pltpu.SemaphoreType.DMA
    anywhere = pl.BlockSpec(memory_space=pl.ANY)
    inside = pl.BlockSpec(memory_space=pltpu.VMEM)
    shapes = ((BASINS, 8, LAYERS), (8, BASINS), (NBANDS, MEMBERS, MEMBERS))
    outs = pl.pallas_call(
        kernel,
        out_shape=tuple(pltpu.VMEM(s, F32) for s in shapes),
        in_specs=[anywhere] * 5,
        out_specs=(inside, inside, inside),
        scratch_shapes=[
            vmem(big, LANES), vmem(big, LANES), vmem(big, LANES),
            pltpu.VMEM((COLS * 8, LANES), jnp.int32),
            pltpu.VMEM((8, LANES), jnp.int32),
            vmem(COLS * BASINS, 8, LANES),
            vmem(COLS, 8, LANES),
            vmem(MINE, 2, LAYERS // 2, ROWS, 8, LANES),
            vmem(MINE, LAYERS // 2, ROWS, 8, LANES),
            vmem(MINE, LAYERS // 2, ROWS, 8, LANES),
            vmem(MINE, ROWS, 8, LANES),
            vmem(MINE, ROWS, 8, LANES),
            vmem(MINE, 2, ROWS, 8, LANES),
            vmem(MINE, 2, ROWS, 8, LANES),
            vmem(MINE, 2, ROWS, 8, LANES),
            vmem(MINE * SPREAD * PAD, LANES),
            vmem(MINE * SPREAD * PAD, LANES),
            vmem(len(TURNED) * SPREAD * WIDE, LANES),
            vmem(len(TURNED) * SPREAD * WIDE, LANES),
            vmem(BASINS * MEMBERS, LANES),
            vmem(PEERS * PAD, LANES),
            vmem(PEERS * PAD, LANES),
            vmem(PAD, LANES),
            vmem(SPREAD * PAD, LANES),
            vmem(PAD, LANES),
            vmem(PEERS * PAD, LANES),
            vmem(PAD, LANES),
            vmem(PEERS * 2 * PAD, LANES),
            dma((MINE,)), dma((2,)),
            dma, dma((MINE,)),
            dma, dma((MINE, 3)),
            dma, dma((MINE,)),
            dma, dma, dma, dma, dma, dma,
        ],
        compiler_params=pltpu.CompilerParams(
            collective_id=0, has_side_effects=True, vmem_limit_bytes=60 << 20
        ),
        name="overturning",
    )(lat_tiles(v), lat_tiles(h), lat_tiles(t), lat_tiles(lab), zone.reshape(8, LANES))
    psi, heat, cov = pl.pallas_call(
        finish,
        out_shape=tuple(jax.ShapeDtypeStruct(s, F32) for s in shapes),
        in_specs=[inside] * 3,
        out_specs=(anywhere,) * 3,
        scratch_shapes=[dma((3,))],
        compiler_params=pltpu.CompilerParams(vmem_limit_bytes=1 << 20),
        name="finish",
    )(*outs)
    return jnp.swapaxes(psi, 1, 2), jnp.swapaxes(heat, 0, 1), cov


def solution(mesh):
    return jax.shard_map(
        local,
        mesh=mesh,
        in_specs=(
            P("member", None, "tile", None),
            P("member", None, "tile", None),
            P("member", None, "tile", None),
            P("tile", None),
            P(),
        ),
        out_specs=(
            P(None, None, ("member", "tile")),
            P(None, ("member", "tile")),
            P(),
        ),
        check_vma=False,
    )
```
